32 devices in a mesh: dp: 2 (over x), tm: 4 (over z), mp: 4 (over y, core).
Axes of the slice: x: 2, y: 2, z: 4, core: 2. Of those that a mesh axis runs over, the one named last changes fastest.
Arguments:
- features: bfloat16 [32, 576, 1024], P(('dp', 'tm'), 'mp'), parts along dimension 0, may hold values from -6 to 6
- queries: bfloat16 [2048, 1024], P(('dp', 'tm')), parts along dimension 0, may hold values from -6 to 6
- anchor_frame: int32 [2048], P(('dp', 'tm')), parts along dimension 0, may hold values from 0 to 15, as said below
- anchor_patch: int32 [2048], P(('dp', 'tm')), parts along dimension 0, may hold values from 0 to 575
- time_offset: float32 [2048, 8, 4], P(('dp', 'tm')), parts along dimension 0, may hold values from -1.99 to 1.99
- space_offset: float32 [2, 2048, 8, 4], P(None, ('dp', 'tm')), parts along dimension 1, may hold values from -3 to 3
- value_weight: bfloat16 [1024, 1024], replicated, may hold values from -0.1875 to 0.1875
- point_weight: bfloat16 [1024, 32], replicated, may hold values from -0.1875 to 0.1875
- point_bias: float32 [32], replicated, may hold values from -6 to 260
- output_weight: bfloat16 [1024, 1024], P('mp'), may hold values from -0.1875 to 0.1875
- project_weight: bfloat16 [1024, 3584], P(None, 'mp'), may hold values from -2 to 2
- norm_gain: float32 [3584], P('mp'), may hold values from 0.1 to 1.9
- query_weight: bfloat16 [3584, 3072], P(None, 'mp'), may hold values from -0.09375 to 0.09375
- query_bias: float32 [3072], P('mp'), may hold values from -6 to 40
- cache_weight: bfloat16 [3584, 1024], P(None, 'mp'), may hold values from -0.09375 to 0.09375
- cache_bias: float32 [1024], P('mp'), may hold values from -6 to 40
Outputs:
- attention: bfloat16 [2048, 3072], P(('dp', 'tm'), 'mp'), parts along dimension 0
- key_value: bfloat16 [2048, 1024], P(('dp', 'tm'), 'mp'), parts along dimension 0
The draws below stay inside these ranges and needn't reach their ends.
There are 2 independent parts, one for each index of `dp`. The reference program is written for one: setup_inputs(seed, part) draws one part's arguments, and reference() takes and returns one part's arrays. A program takes and returns all parts, laid end to end along the dimension named above; an argument that names none is the same for every part. Nothing has to cross between parts.
Inputs may be any that keep to these rules, and one draw needn't show every extreme that they name: `anchor_frame`: the anchor frame of query q lies among the 4 frames that begin at (q // 256) * 4.
All inputs are finite; a program needn't handle non-finite values.
Results may differ from the reference program's by a relative error of at most 0.04.
Values may be sent and summed in bfloat16 or wider, within the bound.
A program may use at most 64 MiB of HBM per device.

```python
import math
import jax
import jax.numpy as jnp
from jax import lax

C = 1024
AH = 8
AHD = 128
POINTS = 4
GRID = 24
PATCH = 576
D = 3584
HEADS = 24
KVH = 4
HD = 128
GROUP = 7
FR_DEV = 4
Q_DEV = 256
FRAMES = 16
QUERIES = 1024


def draw_queries(key, part):
    normal_part = jnp.clip(jax.random.normal(key, (QUERIES, C), jnp.float32), -6.0, 6.0)
    normal_part = normal_part * 0.3
    return normal_part.astype(jnp.bfloat16)


def draw_anchor_frame(key, part):
    position = jnp.arange(QUERIES, dtype=jnp.int32)
    within = jax.random.randint(key, (QUERIES,), 0, FR_DEV, dtype=jnp.int32)
    return position // Q_DEV * FR_DEV + within


def draw_point_bias(key, part):
    normal_part = jnp.clip(jax.random.normal(key, (AH, POINTS), jnp.float32), -6.0, 6.0)
    return normal_part.reshape(AH * POINTS)


def draw_project_weight(key, part):
    normal_part = jnp.clip(jax.random.normal(key, (C, D), jnp.float32), -6.0, 6.0) / math.sqrt(C)
    column_scale = 1.0 + 4.0 * jnp.arange(D, dtype=jnp.float32) / D
    return jnp.clip(normal_part * column_scale[None, :], -2.0, 2.0).astype(jnp.bfloat16)


def draw_query_bias(key, part):
    normal_part = jnp.clip(jax.random.normal(jax.random.fold_in(key, 1), (HEADS, HD), jnp.float32), -6.0, 6.0)
    return normal_part.reshape(HEADS * HD)


def draw_cache_bias(key, part):
    normal_part = jnp.clip(jax.random.normal(jax.random.fold_in(key, 2), (2 * KVH, HD), jnp.float32), -6.0, 6.0)
    return normal_part.reshape(2 * KVH * HD)


def touch_ends(entries, rng, least, largest):
    place = [jax.random.randint(jax.random.fold_in(rng, axis), (), 0, length) for axis, length in enumerate(entries.shape)]
    longest = entries.shape.index(max(entries.shape))
    beside = place[:longest] + [(place[longest] + 1) % entries.shape[longest]] + place[longest + 1:]
    return entries.at[tuple(place)].set(least).at[tuple(beside)].set(largest)


def block_levels(own_key, extent, shards, low, top_value):
    loudness, own = 1.0, jax.random.fold_in(own_key, 6)
    for dim, blocks in shards:
        steps = jnp.exp(jax.random.uniform(jax.random.fold_in(own, dim), (blocks,), jnp.float32, low / len(shards), top_value / len(shards)))
        loudness = loudness * jnp.repeat(steps, extent[dim] // blocks).reshape([-1 if axis == dim else 1 for axis in range(len(extent))])
    return loudness


def gaussian(key, shape, width, most, split=(), kind=jnp.bfloat16):
    values = jax.random.normal(key, shape, jnp.float32) * width
    if len(split) > 0:
        values = block_levels(key, shape, split, -0.22, 0.18) * values
    return jnp.clip(values, min=-most, max=most).astype(kind)


def setup_inputs(seed: int = 0, part: int = 0) -> dict:
    seeds = jax.random.split(jax.random.key(seed), 17)
    part_splits = jax.random.split(jax.random.fold_in(seeds[16], part), 17)
    return {
        "features": gaussian(part_splits[0], (FRAMES, PATCH, C), 1.0, 6.0, ((0, 4), (1, 4))),
        "queries": draw_queries(jax.random.fold_in(jax.random.fold_in(seeds[16], part), 71), part),
        "anchor_frame": draw_anchor_frame(jax.random.fold_in(jax.random.fold_in(seeds[16], part), 71), part),
        "anchor_patch": touch_ends(jax.random.randint(part_splits[3], (QUERIES,), 0, PATCH), jax.random.fold_in(part_splits[3], 1), 0, PATCH - 1).astype(jnp.int32),
        "time_offset": jnp.clip(jax.random.uniform(part_splits[4], (QUERIES, AH, POINTS), jnp.float32, -1.99, 1.99) * block_levels(part_splits[4], (QUERIES, AH, POINTS), ((0, 4),), -0.4, 0.0), -1.99, 1.99),
        "space_offset": jnp.clip(jax.random.uniform(part_splits[5], (2, QUERIES, AH, POINTS), jnp.float32, -3.0, 3.0) * block_levels(part_splits[5], (2, QUERIES, AH, POINTS), ((1, 4),), -0.4, 0.0), -3.0, 3.0),
        "value_weight": gaussian(seeds[6], (C, C), C ** -0.5, 0.1875),
        "point_weight": gaussian(seeds[7], (C, AH * POINTS), C ** -0.5, 0.1875),
        "point_bias": draw_point_bias(jax.random.fold_in(seeds[16], 71), part),
        "output_weight": gaussian(seeds[9], (C, C), C ** -0.5, 0.1875, ((0, 4),)),
        "project_weight": draw_project_weight(jax.random.fold_in(seeds[16], 71), part),
        "norm_gain": jnp.clip(1.0 + 0.18 * jax.random.normal(seeds[11], (D,), jnp.float32), 0.1, 1.9),
        "query_weight": gaussian(seeds[12], (D, HEADS * HD), D ** -0.5, 0.09375, ((1, 4),)),
        "query_bias": draw_query_bias(jax.random.fold_in(seeds[16], 71), part),
        "cache_weight": gaussian(seeds[14], (D, 2 * KVH * HD), D ** -0.5, 0.09375, ((1, 4),)),
        "cache_bias": draw_cache_bias(jax.random.fold_in(seeds[16], 71), part),
    }


rope_base = 1000000.0
epsilon = 1e-06
masked = -1e+30

def rotate(vectors, positions):
    half_width = vectors.shape[-1] // 2
    frequency = rope_base ** (-2.0 * jnp.arange(half_width, dtype=jnp.float32) / vectors.shape[-1])
    angles = positions.astype(jnp.float32)[:, None] * frequency[None, :]
    cosine = jnp.cos(angles)[:, None, :]
    sine_part = jnp.sin(angles)[:, None, :]
    first_half = vectors[..., :half_width]
    second_half = vectors[..., half_width:]
    return jnp.concatenate([first_half * cosine - second_half * sine_part, second_half * cosine + first_half * sine_part], axis=-1)

def trilinear_corners(frame_pos, row_pos, column_pos, weight, frame_total, side):
    floor_frame = jnp.floor(frame_pos)
    floor_row = jnp.floor(row_pos)
    floor_column = jnp.floor(column_pos)
    frame_part = frame_pos - floor_frame
    row_part = row_pos - floor_row
    column_part = column_pos - floor_column
    frame_start = floor_frame.astype(jnp.int32)
    row_start = floor_row.astype(jnp.int32)
    column_start = floor_column.astype(jnp.int32)
    listing = []
    for frame_step in (0, 1):
        for row_step in (0, 1):
            for column_step in (0, 1):
                frame_cell = frame_start + frame_step
                row_cell = row_start + row_step
                column_cell = column_start + column_step
                portion = weight * (frame_part if frame_step else 1.0 - frame_part)
                portion = portion * (row_part if row_step else 1.0 - row_part)
                portion = portion * (column_part if column_step else 1.0 - column_part)
                inside = (frame_cell >= 0) & (frame_cell < frame_total) & (row_cell >= 0) & (row_cell < side)
                inside = inside & (column_cell >= 0) & (column_cell < side)
                portion = jnp.where(inside, portion, 0.0)
                patch_id = jnp.clip(row_cell, 0, side - 1) * side + jnp.clip(column_cell, 0, side - 1)
                listing.append((frame_cell, patch_id.astype(jnp.int32), portion))
    return listing

def reference(features, queries, anchor_frame, anchor_patch, time_offset, space_offset, value_weight, point_weight, point_bias, output_weight, project_weight, norm_gain, query_weight, query_bias, cache_weight, cache_bias):
    patch_values = jnp.dot(features.reshape(FRAMES * PATCH, C), value_weight, preferred_element_type=jnp.float32).astype(jnp.bfloat16)
    by_head = patch_values.reshape(FRAMES * PATCH, AH, AHD).transpose(1, 0, 2)
    logits = jnp.dot(queries, point_weight, preferred_element_type=jnp.float32) + point_bias
    point_share = jax.nn.softmax(logits.reshape(QUERIES, AH, POINTS), axis=-1)
    frame_pos = anchor_frame.astype(jnp.float32)[:, None, None] + time_offset
    row_pos = (anchor_patch // GRID).astype(jnp.float32)[:, None, None] + space_offset[0]
    column_pos = (anchor_patch % GRID).astype(jnp.float32)[:, None, None] + space_offset[1]

    def sample_head(inputs):
        lookup, frame_head, row_head, column_head, share_head = inputs
        running = jnp.zeros((QUERIES, AHD), jnp.float32)
        for frame_cell, patch_id, portion in trilinear_corners(frame_head, row_head, column_head, share_head, FRAMES, GRID):
            picked = lookup[jnp.clip(frame_cell, 0, FRAMES - 1) * PATCH + patch_id]
            running = running + lax.optimization_barrier(jnp.sum(portion[..., None] * picked.astype(jnp.float32), axis=1))
        return running
    sampled = lax.map(sample_head, (by_head, frame_pos.transpose(1, 0, 2), row_pos.transpose(1, 0, 2), column_pos.transpose(1, 0, 2), point_share.transpose(1, 0, 2)))
    sampled = sampled.transpose(1, 0, 2).reshape(QUERIES, C).astype(jnp.bfloat16)
    abstract = (queries.astype(jnp.float32) + jnp.dot(sampled, output_weight, preferred_element_type=jnp.float32)).astype(jnp.bfloat16)
    visual = jnp.dot(abstract, project_weight, preferred_element_type=jnp.float32)
    normed = (visual * lax.rsqrt(lax.optimization_barrier(jnp.mean(visual * visual, axis=1, keepdims=True)) + epsilon) * norm_gain).astype(jnp.bfloat16)
    positions = jnp.arange(QUERIES, dtype=jnp.int32)
    query_state = (jnp.dot(normed, query_weight, preferred_element_type=jnp.float32) + query_bias).reshape(QUERIES, HEADS, HD)
    query_state = rotate(query_state, positions).astype(jnp.bfloat16)
    cache_state = (jnp.dot(normed, cache_weight, preferred_element_type=jnp.float32) + cache_bias).reshape(QUERIES, 2 * KVH, HD)
    cache_state = jnp.concatenate([rotate(cache_state[:, :KVH], positions), cache_state[:, KVH:]], axis=1)
    key_value = cache_state.reshape(QUERIES, 2 * KVH * HD).astype(jnp.bfloat16)
    key_heads = key_value.reshape(QUERIES, 2 * KVH, HD).transpose(1, 0, 2)
    query_heads = query_state.transpose(1, 0, 2)
    allowed = positions[None, :] <= positions[:, None]

    def attend_head(head_id):
        group_id = head_id // GROUP
        scores = jnp.dot(query_heads[head_id], key_heads[group_id].T, preferred_element_type=jnp.float32) * HD ** (-0.5)
        scores = jnp.where(allowed, scores, masked)
        row_peak = lax.optimization_barrier(jnp.max(scores, axis=1, keepdims=True))
        weights = jnp.where(allowed, jnp.exp(scores - row_peak), 0.0)
        weighted = jnp.dot(weights.astype(jnp.bfloat16), key_heads[KVH + group_id], preferred_element_type=jnp.float32)
        return weighted / lax.optimization_barrier(jnp.sum(weights, axis=1, keepdims=True))
    attention = lax.map(attend_head, jnp.arange(HEADS, dtype=jnp.int32))
    attention = attention.transpose(1, 0, 2).reshape(QUERIES, HEADS * HD).astype(jnp.bfloat16)
    return (attention, key_value)
```

```python
import functools

import jax
import jax.numpy as jnp
from jax import lax
from jax.experimental import pallas as pl
from jax.experimental.pallas import tpu as pltpu
from jax.sharding import PartitionSpec as P

AH = 8
POINTS = 4
GRID = 24
KVH = 4
HD = 128
GROUP = 7

rope_base = 1000000.0
epsilon = 1e-06
masked = -1e30
MESH = pl.DeviceIdType.MESH
BF = jnp.bfloat16
F32 = jnp.float32


def remote(src, dst, send, recv, device):
    return pltpu.make_async_remote_copy(
        src_ref=src, dst_ref=dst, send_sem=send, recv_sem=recv, device_id=device, device_id_type=MESH
    )


class Gather:
    def __init__(self, slot_ref, own, sems, groups, me):
        self.chips = groups // 2
        self.chip, self.core = me // 2, me % 2
        self.me, self.partner = me, me + 1 - 2 * (me % 2)
        cs, cr, ps, pr = sems
        self.cross = [None] + [
            remote(
                own,
                slot_ref(me),
                cs(d),
                cr(d),
                {"mp": (self.chip + d) % self.chips * 2 + self.core},
            )
            for d in range(1, self.chips)
        ]
        self.near = [remote(own, slot_ref(me), ps(0), pr(0), {"mp": self.partner})]
        for d in range(1, self.chips):
            slot = slot_ref(self.slot(d, self.core))
            self.near.append(remote(slot, slot, ps(d), pr(d), {"mp": self.partner}))

    def slot(self, d, core):
        return (self.chip + self.chips - d) % self.chips * 2 + core

    def start(self):
        for copy in self.cross[1:]:
            copy.start()
        self.near[0].start()

    def arrivals(self):
        self.near[0].wait_recv()
        yield self.partner
        for d in range(1, self.chips):
            self.cross[d].wait_recv()
            self.near[d].start()
            yield self.slot(d, self.core)
            self.near[d].wait_recv()
            yield self.slot(d, 1 - self.core)

    def drain(self):
        for copy in self.cross[1:] + self.near:
            copy.wait_send()


def kernel(
    groups,
    spans,
    frames,
    features,
    queries,
    coords,
    cosine,
    sine,
    gain,
    query_bias,
    cache_bias,
    value_hbm,
    output_hbm,
    project_hbm,
    query_hbm,
    cache_hbm,
    attention,
    key_value,
    vw,
    wo,
    wp,
    wq,
    wc,
    halo,
    own_values,
    halo_values,
    corner,
    partial,
    rs_send,
    rs_recv,
    ab,
    vx,
    ssq,
    q_acc,
    kv_acc,
    qs,
    kv,
    peak,
    denom,
    numer,
    load_sem,
    halo_send,
    halo_recv,
    rs_ss,
    rs_rs,
    sq_ss,
    sq_rs,
    z_ss,
    z_rs,
    ag_sem,
):
    me = lax.axis_index("mp")
    t = lax.axis_index("tm")
    cells, width = features.shape
    rows = queries.shape[0]
    half = 2 * (cells // frames)
    lines = cells // frames // GRID
    piece = rows // groups
    model = wp.shape[1]
    q_heads = qs.shape[0]
    ch = kv.shape[3] // HD

    loads = [
        pltpu.make_async_copy(src, dst, load_sem.at[i])
        for i, (src, dst) in enumerate(
            [
                (value_hbm, vw),
                (output_hbm, wo.at[me]),
                (project_hbm, wp),
                (cache_hbm, wc),
                (query_hbm, wq),
            ]
        )
    ]
    for load in loads:
        load.start()

    barrier = pltpu.get_barrier_semaphore()
    for d in range(1, groups):
        pl.semaphore_signal(barrier, inc=1, device_id={"mp": (me + d) % groups}, device_id_type=MESH)
    for d in range(1, spans):
        pl.semaphore_signal(barrier, inc=1, device_id={"tm": (t + d) % spans}, device_id_type=MESH)
    pl.semaphore_wait(barrier, groups + spans - 2)

    low, high = halo.at[pl.ds(0, half)], halo.at[pl.ds(half, half)]
    up = remote(
        features.at[pl.ds(cells - half, half)], low, halo_send.at[0], halo_recv.at[0], {"tm": (t + 1) % spans}
    )
    down = remote(
        features.at[pl.ds(0, half)],
        high,
        halo_send.at[1],
        halo_recv.at[1],
        {"tm": (t + spans - 1) % spans},
    )

    @pl.when(t < spans - 1)
    def _():
        up.start()

    @pl.when(t > 0)
    def _():
        down.start()

    @pl.when(t == 0)
    def _():
        halo[pl.ds(0, half), :] = jnp.zeros((half, width), BF)

    @pl.when(t == spans - 1)
    def _():
        halo[pl.ds(half, half), :] = jnp.zeros((half, width), BF)

    def gather_sems(index):
        return [functools.partial(lambda k, d: ag_sem.at[index, k, d], k) for k in range(4)]

    wo_gather = Gather(lambda s: wo.at[s], output_hbm, gather_sems(0), groups, me)
    wo_gather.start()

    loads[0].wait()

    def project_values(source, target):
        @pl.loop(0, width // 256)
        def _(c):
            cols = pl.ds(pl.multiple_of(c * 256, 256), 256)
            target[:, cols] = jnp.dot(
                source[...], vw[:, cols], preferred_element_type=F32
            ).astype(BF)

    line_index = lax.broadcasted_iota(jnp.int32, (GRID, rows), 0).astype(F32)
    first_line = (me * lines).astype(F32)
    first_frame = (t * frames).astype(F32)

    def hat(position, cell):
        return jnp.maximum(1.0 - jnp.abs(position - cell), 0.0)

    def sample(values, offsets, head):
        info = coords[head]
        columns = [hat(info[8 + k : 9 + k], line_index) for k in range(POINTS)]
        for f, offset in enumerate(offsets):
            timed = info[12:16] * hat(info[0:4], first_frame + offset)
            for line in range(lines):
                share = timed * hat(info[4:8], first_line + line)
                total = share[0:1] * columns[0]
                for k in range(1, POINTS):
                    total = total + share[k : k + 1] * columns[k]
                corner[pl.ds((f * lines + line) * GRID, GRID), :] = total
        cols = pl.ds(pl.multiple_of(head * HD, HD), HD)
        return lax.dot_general(
            corner[pl.ds(0, values.shape[0]), :].astype(BF),
            values[:, cols],
            (((0,), (0,)), ((), ())),
            preferred_element_type=F32,
        )

    project_values(features, own_values)

    @pl.loop(0, AH)
    def _(head):
        cols = pl.ds(pl.multiple_of(head * HD, HD), HD)
        partial[:, cols] = sample(own_values, range(frames), head)

    @pl.when(t > 0)
    def _():
        up.wait_recv()

    @pl.when(t < spans - 1)
    def _():
        down.wait_recv()

    project_values(halo, halo_values)

    @pl.loop(0, AH)
    def _(head):
        cols = pl.ds(pl.multiple_of(head * HD, HD), HD)
        total = partial[:, cols] + sample(halo_values, (-2, -1, frames, frames + 1), head)
        rs_send[:, :, cols] = total.reshape(groups, piece, HD).astype(BF)

    rs = []
    for d in range(1, groups):
        peer = (me + d) % groups
        copy = remote(rs_send.at[peer], rs_recv.at[d], rs_ss.at[d], rs_rs.at[d], {"mp": peer})
        copy.start()
        rs.append(copy)

    loads[1].wait()
    for _ in wo_gather.arrivals():
        pass

    total = rs_send[me].astype(F32)
    for d in range(1, groups):
        rs[d - 1].wait_recv()
        total = total + rs_recv[d].astype(F32)
    mixed = jnp.dot(total.astype(BF), wo[...].reshape(width, width), preferred_element_type=F32)
    own_rows = pl.ds(pl.multiple_of(me * piece, piece), piece)
    ab[me] = (queries[own_rows, :].astype(F32) + mixed).astype(BF)
    ab_gather = Gather(lambda s: ab.at[s], ab.at[me], gather_sems(1), groups, me)
    ab_gather.start()
    loads[2].wait()
    for _ in ab_gather.arrivals():
        pass

    visual = jnp.dot(ab[...].reshape(rows, width), wp[...], preferred_element_type=F32)
    vx[me] = (visual * gain[...]).astype(BF)
    vx_gather = Gather(lambda s: vx.at[s], vx.at[me], gather_sems(2), groups, me)
    vx_gather.start()
    squares = jnp.broadcast_to(jnp.sum(visual * visual, axis=1, keepdims=True), (rows, HD)).T
    ssq[0] = squares[0:8]
    sq = []
    for d in range(1, groups):
        copy = remote(
            ssq.at[0], ssq.at[d], sq_ss.at[d], sq_rs.at[d], {"mp": (me + d) % groups}
        )
        copy.start()
        sq.append(copy)

    q_width = wq.shape[1]
    tile = 256 if q_width % 256 == 0 else 128

    def slot_rows(slot):
        return pl.ds(pl.multiple_of(slot * model, 64), model)

    def add_cache(slot, first):
        term = jnp.dot(vx[slot], wc[slot_rows(slot), :], preferred_element_type=F32)
        kv_acc[...] = term if first else kv_acc[...] + term

    def add_query(slot, first):
        @pl.loop(0, q_width // tile)
        def _(c):
            cols = pl.ds(pl.multiple_of(c * tile, tile), tile)
            term = jnp.dot(vx[slot], wq[slot_rows(slot), cols], preferred_element_type=F32)
            q_acc[:, cols] = term if first else q_acc[:, cols] + term

    loads[3].wait()
    loads[4].wait()
    add_cache(me, True)
    add_query(me, True)
    for order, slot in enumerate(vx_gather.arrivals()):
        add_cache(slot, False)
        if order < groups - 2:
            add_query(slot, False)
        last = slot

    square_sum = ssq[0]
    for d in range(1, groups):
        sq[d - 1].wait_recv()
        square_sum = square_sum + ssq[d]
    scale_row = lax.rsqrt(square_sum * (1.0 / (model * groups)) + epsilon)
    scale = jnp.broadcast_to(scale_row[0:1], (HD, rows)).T

    def turn(x, cos, sin):
        return x * cos + pltpu.roll(x, HD // 2, 1) * sin

    for i in range(ch):
        is_key = me * ch + i < KVH
        cols = slice(i * HD, (i + 1) * HD)
        state = kv_acc[:, cols] * scale + cache_bias[:, cols]
        cos = jnp.where(is_key, cosine[...], 1.0)
        sin = jnp.where(is_key, sine[...], 0.0)
        state = turn(state, cos, sin).astype(BF)
        kv[t, me, :, cols] = state
        key_value[:, cols] = state

    mine = kv.at[t, me]
    z_copies = []
    for d in range(1, spans):
        z_copies.append(remote(mine, mine, z_ss.at[d], z_rs.at[d], {"tm": (t + d) % spans}))

        @pl.when(t + d < spans)
        def _(d=d):
            z_copies[d - 1].start()

    def block_gather(d):
        j = lax.rem(t + spans - d, spans)
        return j, Gather(lambda s: kv.at[j, s], kv.at[j, me], gather_sems(3 + d), groups, me)

    own_gather = block_gather(0)
    own_gather[1].start()
    add_query(last, False)
    for i in range(q_heads):
        cols = slice(i * HD, (i + 1) * HD)
        state = q_acc[:, cols] * scale + query_bias[:, cols]
        qs[i] = turn(state, cosine[...], sine[...]).astype(BF)

    def attend(j, diagonal):
        @pl.loop(0, q_heads)
        def _(i):
            g = (me * q_heads + i) // GROUP
            k_cols = pl.ds(pl.multiple_of(lax.rem(g, ch) * HD, HD), HD)
            keys = kv[j, g // ch, :, k_cols]
            values = kv[j, (KVH + g) // ch, :, pl.ds(pl.multiple_of(lax.rem(KVH + g, ch) * HD, HD), HD)]
            scores = lax.dot_general(
                qs[i], keys, (((1,), (1,)), ((), ())), preferred_element_type=F32
            ) * (HD ** -0.5)
            if diagonal:
                q_pos = lax.broadcasted_iota(jnp.int32, (rows, rows), 0)
                k_pos = lax.broadcasted_iota(jnp.int32, (rows, rows), 1)
                scores = jnp.where(k_pos <= q_pos, scores, masked)
            top = jnp.max(scores, axis=1, keepdims=True)
            if diagonal:
                new_peak = jnp.broadcast_to(top, (rows, HD))
            else:
                new_peak = jnp.maximum(peak[i], top)
            weights = jnp.exp(scores - new_peak[:, 0:1])
            added = jnp.sum(weights, axis=1, keepdims=True)
            product = jnp.dot(weights.astype(BF), values, preferred_element_type=F32)
            if diagonal:
                denom[i] = jnp.broadcast_to(added, (rows, HD))
                numer[i] = product
            else:
                rescale = jnp.exp(peak[i] - new_peak)
                denom[i] = denom[i] * rescale + added
                numer[i] = numer[i] * rescale + product
            peak[i] = new_peak

    for _ in own_gather[1].arrivals():
        pass
    attend(t, True)
    for d in range(1, spans):

        @pl.when(t >= d)
        def _(d=d):
            j, gather = block_gather(d)
            arrived = kv.at[j, me]
            remote(arrived, arrived, z_ss.at[d], z_rs.at[d], {"tm": t}).wait_recv()
            gather.start()
            for _ in gather.arrivals():
                pass
            attend(j, False)
            gather.drain()

    for i in range(q_heads):
        attention[:, i * HD : (i + 1) * HD] = (numer[i] / denom[i]).astype(BF)

    @pl.when(t < spans - 1)
    def _():
        up.wait_send()

    @pl.when(t > 0)
    def _():
        down.wait_send()

    for gather in (wo_gather, ab_gather, vx_gather, own_gather[1]):
        gather.drain()
    for copy in rs + sq:
        copy.wait_send()
    for d in range(1, spans):

        @pl.when(t + d < spans)
        def _(d=d):
            z_copies[d - 1].wait_send()


def local(
    features,
    queries,
    anchor_frame,
    anchor_patch,
    time_offset,
    space_offset,
    value_weight,
    point_weight,
    point_bias,
    output_weight,
    project_weight,
    norm_gain,
    query_weight,
    query_bias,
    cache_weight,
    cache_bias,
):
    groups = lax.axis_size("mp")
    spans = lax.axis_size("tm")
    frames_here, patches_here, width = features.shape
    cells = frames_here * patches_here
    rows = queries.shape[0]
    logits = jnp.dot(queries, point_weight, preferred_element_type=F32) + point_bias
    share = jax.nn.softmax(logits.reshape(rows, AH, POINTS), axis=-1)
    frame_pos = anchor_frame.astype(F32)[:, None, None] + time_offset
    row_pos = (anchor_patch // GRID).astype(F32)[:, None, None] + space_offset[0]
    column_pos = (anchor_patch % GRID).astype(F32)[:, None, None] + space_offset[1]
    coords = jnp.stack([frame_pos, row_pos, column_pos, share], axis=0)
    coords = coords.transpose(2, 0, 3, 1).reshape(AH, 4 * POINTS, rows)
    positions = lax.axis_index("tm") * rows + jnp.arange(rows, dtype=jnp.int32)
    frequency = rope_base ** (-2.0 * jnp.arange(HD // 2, dtype=F32) / HD)
    angles = positions.astype(F32)[:, None] * frequency[None, :]
    cosine = jnp.cos(angles)
    sine = jnp.sin(angles)
    cosine = jnp.concatenate([cosine, cosine], axis=1)
    sine = jnp.concatenate([-sine, sine], axis=1)
    model = project_weight.shape[1]
    q_width = query_weight.shape[1]
    c_width = cache_weight.shape[1]
    q_heads = q_width // HD
    piece = rows // groups
    chips = groups // 2
    vmem = pl.BlockSpec(memory_space=pltpu.VMEM)
    hbm = pl.BlockSpec(memory_space=pl.ANY)
    dma = pltpu.SemaphoreType.DMA
    V = pltpu.VMEM
    return tuple(
        pl.pallas_call(
            functools.partial(kernel, groups, spans, frames_here),
            out_shape=(
                jax.ShapeDtypeStruct((rows, q_width), BF),
                jax.ShapeDtypeStruct((rows, c_width), BF),
            ),
            in_specs=[vmem] * 8 + [hbm] * 5,
            out_specs=(vmem, vmem),
            scratch_shapes=[
                V((width, width), BF),
                V((groups, width // groups, width), BF),
                V((width, model), BF),
                V(query_weight.shape, BF),
                V(cache_weight.shape, BF),
                V((4 * patches_here, width), BF),
                V((cells, width), BF),
                V((4 * patches_here, width), BF),
                V((max(4, frames_here) * patches_here, rows), F32),
                V((rows, width), F32),
                V((groups, piece, width), BF),
                V((groups, piece, width), BF),
                V((groups, piece, width), BF),
                V((groups, rows, model), BF),
                V((groups, 8, rows), F32),
                V((rows, q_width), F32),
                V((rows, c_width), F32),
                V((q_heads, rows, HD), BF),
                V((spans, groups, rows, c_width), BF),
                V((q_heads, rows, HD), F32),
                V((q_heads, rows, HD), F32),
                V((q_heads, rows, HD), F32),
                dma((5,)),
                dma((2,)),
                dma((2,)),
                dma((groups,)),
                dma((groups,)),
                dma((groups,)),
                dma((groups,)),
                dma((spans,)),
                dma((spans,)),
                dma((3 + spans, 4, chips)),
            ],
            compiler_params=pltpu.CompilerParams(
                collective_id=0, has_side_effects=True, vmem_limit_bytes=60 * 1024 * 1024
            ),
        )(
            features.reshape(cells, width),
            queries,
            coords,
            cosine,
            sine,
            norm_gain[None],
            query_bias[None],
            cache_bias[None],
            value_weight,
            output_weight,
            project_weight,
            query_weight,
            cache_weight,
        )
    )


def solution(mesh):
    return jax.shard_map(
        local,
        mesh=mesh,
        in_specs=(
            P(("dp", "tm"), "mp", None),
            P(("dp", "tm"), None),
            P(("dp", "tm")),
            P(("dp", "tm")),
            P(("dp", "tm"), None, None),
            P(None, ("dp", "tm"), None, None),
            P(),
            P(),
            P(),
            P("mp", None),
            P(None, "mp"),
            P("mp"),
            P(None, "mp"),
            P("mp"),
            P(None, "mp"),
            P("mp"),
        ),
        out_specs=(P(("dp", "tm"), "mp"), P(("dp", "tm"), "mp")),
        check_vma=False,
    )
```
